512 devices in a mesh: group: 8 (over x, y_hi), vocab: 64 (over z, y_lo, core).
Axes of the slice: x: 4, y: 4 (y_hi: 2, y_lo: 2; y = y_hi * 2 + y_lo), z: 16, core: 2. Of those that a mesh axis runs over, the one named last changes fastest.
Arguments:
- table: bfloat16 [4608, 196608], P('vocab', 'group')
- hidden: bfloat16 [448, 4608], P(None, 'vocab')
- gain: bfloat16 [4608], P('vocab'), may hold values from 0.099609375 to 1.8984375
- ids: int32 [448], replicated, may hold values from 0 to 196607
Outputs:
- next_embed: bfloat16 [448, 4608], P(None, 'vocab')
- logprobs: float32 [448, 196608], P(None, ('group', 'vocab'))
- chosen: float32 [448], replicated
The draws below stay inside these ranges and needn't reach their ends.
All inputs are finite; a program needn't handle non-finite values.
Results may differ from the reference program's by a relative error of at most 0.001.
Values may be sent and summed in bfloat16 or wider, within the bound.
No kernel may reach another device: no remote copies, remote signals or barrier semaphores. Data moves between devices by JAX's collectives and lax.ppermute only.
A program may use at most 64 MiB of HBM per device.

```python
import math
import jax
import jax.numpy as jnp
from jax import lax

D = 4608
TOK = 448
VOCAB = 196608


def draw_table(key, part):
    first, second = jax.random.split(jax.random.fold_in(key, 11))
    place = jnp.arange(VOCAB, dtype=jnp.float32) / VOCAB
    rough = jnp.exp(jax.random.uniform(second, (VOCAB,), jnp.float32, -0.35, 0.35))
    base = jax.random.normal(first, (D, VOCAB), jnp.float32)
    scale = 0.5 * 4.0 ** place * rough
    return (base * scale[None, :] / math.sqrt(D)).astype(jnp.bfloat16)


def draw_hidden(key, part):
    first, second, third = jax.random.split(jax.random.fold_in(key, 23), 3)
    place = jnp.arange(D, dtype=jnp.float32) / D
    rough = jnp.exp(jax.random.uniform(second, (D,), jnp.float32, -0.5, 0.5))
    row_scale = 10.0 ** jax.random.uniform(third, (TOK, 1), jnp.float32, 0.0, 1.0)
    base = jax.random.normal(first, (TOK, D), jnp.float32)
    column = 10.0 ** place * rough
    return (base * column[None, :] * row_scale).astype(jnp.bfloat16)


def touch_ends(result, key, smallest, top_value):
    longest = result.shape.index(max(result.shape))
    spots = []
    for shift in (0, 1):
        where = [jax.random.randint(jax.random.fold_in(key, axis), (), 0, length) for axis, length in enumerate(result.shape)]
        where[longest] = (where[longest] + shift) % result.shape[longest]
        spots.append(tuple(where))
    return result.at[spots[0]].set(smallest).at[spots[1]].set(top_value)


def setup_inputs(seed: int = 0) -> dict:
    key_of = jax.random.split(jax.random.key(seed), 5)
    table = draw_table(jax.random.fold_in(key_of[4], 71), 0)
    hidden = draw_hidden(jax.random.fold_in(key_of[4], 71), 0)
    gain = jnp.clip(1.0 + 0.18 * jax.random.normal(key_of[2], (D,), jnp.float32), 0.099609375, 1.8984375).astype(jnp.bfloat16)
    ids = touch_ends(jax.random.randint(key_of[3], (TOK,), 0, VOCAB), jax.random.fold_in(key_of[3], 1), 0, VOCAB - 1).astype(jnp.int32)
    return {"table": table, "hidden": hidden, "gain": gain, "ids": ids}


def reference(table, hidden, gain, ids):
    picked = jnp.take(table, ids, axis=1).astype(jnp.float32).T
    next_embed = (picked * math.sqrt(D)).astype(jnp.bfloat16)
    states = hidden.astype(jnp.float32)
    mean_sq = lax.optimization_barrier(jnp.sum(states * states, axis=1, keepdims=True)) / D
    normed = (states * gain.astype(jnp.float32) * lax.rsqrt(mean_sq + 1e-06)).astype(jnp.bfloat16)
    logits = jnp.dot(normed, table, preferred_element_type=jnp.float32)
    capped = 30.0 * jnp.tanh(logits / 30.0)
    total = lax.optimization_barrier(jnp.sum(jnp.exp(capped), axis=1))
    log_total = jnp.log(total)
    logprobs = capped - log_total[:, None]
    picked_logit = jnp.take_along_axis(capped, ids[:, None].astype(jnp.int32), axis=1)[:, 0]
    chosen = picked_logit - log_total
    return (next_embed, logprobs, chosen)
```

```python
import math

import jax
import jax.numpy as jnp
from jax import lax
from jax.experimental import pallas as pl
from jax.experimental.pallas import tpu as pltpu
from jax.sharding import Mesh
from jax.sharding import PartitionSpec as P

GROUP = ("group_0", "group_1")
FAR = "depth"
NEAR = ("row", "core")
VOCAB = (FAR,) + NEAR
PLANE = GROUP + NEAR
LANES = 512


def copies_of(x, axes):
    many = jnp.broadcast_to(x[None], (lax.axis_size(axes),) + x.shape)
    return lax.all_to_all(many, axes, split_axis=0, concat_axis=0, tiled=True)


def as_rows(x):
    return jnp.pad(x, (0, LANES - x.shape[0])).reshape(LANES // 128, 128)


def arrange(table, places, near_index, near_n):
    share, span_cols = table.shape
    slots = places.shape[0]
    cols = span_cols // (lax.axis_size(FAR) * near_n)

    def kernel(places_ref, near_ref, table_ref, *refs):
        out_refs, sems = refs[:near_n], refs[near_n]
        copies = []
        for k in range(near_n):
            for j in range(slots):
                block = places_ref[j] * near_n + (near_ref[0] ^ k)
                copies.append(
                    pltpu.make_async_copy(
                        table_ref.at[:, pl.ds(pl.multiple_of(block * cols, cols), cols)],
                        out_refs[k].at[:, pl.ds(j * cols, cols)],
                        sems.at[k * slots + j],
                    )
                )
        for c in copies:
            c.start()
        for c in copies:
            c.wait()

    smem, vmem = pl.BlockSpec(memory_space=pltpu.SMEM), pl.BlockSpec(memory_space=pltpu.VMEM)
    return pl.pallas_call(
        kernel,
        in_specs=[smem, smem, pl.BlockSpec(memory_space=pltpu.HBM)],
        out_specs=[vmem] * near_n,
        out_shape=[jax.ShapeDtypeStruct((share, slots * cols), table.dtype)] * near_n,
        scratch_shapes=[pltpu.SemaphoreType.DMA((near_n * slots,))],
    )(places, near_index[None], table)


def add_partial(x, w, slot, cols, received, dtype):
    y = jnp.dot(x, w[:, slot * cols : (slot + 1) * cols], preferred_element_type=jnp.float32)
    for r in received:
        y = y + r.astype(jnp.float32)
    return y.astype(dtype)


def layer(table, hidden, gain, ids):
    share, span_cols = table.shape
    tok = hidden.shape[0]
    far_n, near_n = lax.axis_size(FAR), lax.axis_size(NEAR)
    voc_cols = span_cols // (far_n * near_n)
    width = share * far_n * near_n
    group_index = lax.axis_index(GROUP)
    vocab_index = lax.axis_index(VOCAB)
    depth = lax.axis_index(FAR)
    steps = far_n // 2

    order = []
    for s in range(steps):
        order += [steps - s, (s - steps + 1)]
    places = (depth + jnp.array(order, jnp.int32)) % far_n
    early = far_n // 2

    fill = jnp.broadcast_to(gain[:, None], (share, LANES - tok))
    both = jnp.concatenate([hidden.T, fill], axis=1)
    near_index = lax.axis_index(NEAR)
    first = arrange(table, places[:early], near_index, near_n)
    both = lax.all_gather(both, NEAR, axis=0, tiled=True)
    first, both = lax.optimization_barrier((first, both))
    swapped = jnp.zeros((near_n * share, first[0].shape[1]), table.dtype)
    for k in range(near_n):
        slab = first[k]
        if k:
            slab = lax.ppermute(slab, NEAR, [(i, i ^ k) for i in range(near_n)])
        swapped = lax.dynamic_update_slice(swapped, slab, ((near_index ^ k) * share, 0))
    first = swapped

    both = both.astype(jnp.float32)
    states, gains = both[:, :tok], both[:, tok : tok + 1]
    squares = jnp.sum(states * states, axis=0)
    squares, late_table = lax.optimization_barrier((squares, table))
    squares = copies_of(as_rows(squares), FAR).reshape(far_n, -1, 128)
    mean_sq = squares.sum(axis=0).reshape(LANES)[:tok] / width
    normed = (states * gains * lax.rsqrt(mean_sq + 1e-06)[None, :]).astype(jnp.bfloat16).T

    second = arrange(late_table, places[early:], near_index * 0, near_n)
    second = jnp.stack(second)
    second = lax.all_to_all(second, NEAR, split_axis=0, concat_axis=0, tiled=True)
    second = second.reshape(near_n * share, -1)

    def part(slot, received, dtype=jnp.bfloat16):
        w, at = (first, slot) if slot < early else (second, slot - early)
        return add_partial(normed, w, at, voc_cols, received, dtype)

    ahead = [(i, (i + 1) % far_n) for i in range(far_n)]
    behind = [(i, (i - 1) % far_n) for i in range(far_n)]
    up, down = [], []
    for s in range(steps):
        out = part(2 * s, up)
        up = [lax.ppermute(out, FAR, ahead)]
        if s < steps - 1:
            out = part(2 * s + 1, down)
            down = [lax.ppermute(out, FAR, behind)]
    logits = part(2 * steps - 1, up + down, jnp.float32)

    local_ids = ids - group_index * span_cols
    inside = jnp.logical_and(local_ids >= 0, local_ids < span_cols)
    found = jnp.take(late_table, jnp.clip(local_ids, 0, span_cols - 1), axis=1)
    found = jnp.where(inside[None, :], found, 0)
    found = copies_of(found, GROUP).reshape(-1, share, tok)
    embed = jnp.sum(found.astype(jnp.float32), axis=0)
    next_embed = (embed * math.sqrt(width)).astype(jnp.bfloat16).T

    capped = 30.0 * jnp.tanh(logits / 30.0)
    offsets = ids - (group_index * far_n * near_n + vocab_index) * voc_cols
    columns = lax.broadcasted_iota(jnp.int32, capped.shape, 1)
    pick = jnp.sum(jnp.where(columns == offsets[:, None], capped, 0.0), axis=1)
    sums = jnp.sum(jnp.exp(capped), axis=1)
    pair = jnp.concatenate([as_rows(sums), as_rows(pick)])
    for axes in (PLANE, FAR):
        pair = copies_of(pair, axes).reshape(-1, *pair.shape).sum(axis=0)
    totals, picks = pair.reshape(2, LANES)[:, :tok]
    log_total = jnp.log(totals)
    return (next_embed, capped - log_total[:, None], picks - log_total)


def solution(mesh):
    torus = Mesh(
        mesh.devices.reshape(4, 2, 16, 2, 2),
        GROUP + VOCAB,
    )
    return jax.shard_map(
        layer,
        mesh=torus,
        in_specs=(P(VOCAB, GROUP), P(None, VOCAB), P(VOCAB), P()),
        out_specs=(P(None, VOCAB), P(None, GROUP + VOCAB), P()),
        check_vma=False,
    )
```

```python
import math

import jax
import jax.numpy as jnp
from jax import lax
from jax.experimental import pallas as pl
from jax.experimental.pallas import tpu as pltpu
from jax.sharding import Mesh
from jax.sharding import PartitionSpec as P

GROUP = ("group_0", "group_1")
FAR = "depth"
NEAR = ("row", "core")
VOCAB = (FAR,) + NEAR
PLANE = GROUP + NEAR
LANES = 512


def copies_of(x, axes):
    many = jnp.broadcast_to(x[None], (lax.axis_size(axes),) + x.shape)
    return lax.all_to_all(many, axes, split_axis=0, concat_axis=0, tiled=True)


def as_rows(x):
    return jnp.pad(x, (0, LANES - x.shape[0])).reshape(LANES // 128, 128)


def arrange(table, places, near_index, near_n, joined):
    share, span_cols = table.shape
    cores, slots = places.shape
    per = span_cols // (lax.axis_size(FAR) * near_n)
    cols = per * cores

    def kernel(places_ref, near_ref, table_ref, *refs):
        sems = refs[-1]
        copies = []
        for k in range(near_n):
            out_ref = refs[0].at[k] if joined else refs[k]
            near = near_ref[0] ^ k
            core = near % cores
            for j in range(slots):
                block = places_ref[core * slots + j] * near_n + near - core
                copies.append(
                    pltpu.make_async_copy(
                        table_ref.at[:, pl.ds(pl.multiple_of(block * per, per), cols)],
                        out_ref.at[:, pl.ds(j * cols, cols)],
                        sems.at[k * slots + j],
                    )
                )
        for c in copies:
            c.start()
        for c in copies:
            c.wait()

    smem, vmem = pl.BlockSpec(memory_space=pltpu.SMEM), pl.BlockSpec(memory_space=pltpu.VMEM)
    return pl.pallas_call(
        kernel,
        in_specs=[smem, smem, pl.BlockSpec(memory_space=pltpu.HBM)],
        out_specs=[vmem] * (1 if joined else near_n),
        out_shape=[jax.ShapeDtypeStruct((near_n, share, slots * cols), table.dtype)]
        if joined
        else [jax.ShapeDtypeStruct((share, slots * cols), table.dtype)] * near_n,
        scratch_shapes=[pltpu.SemaphoreType.DMA((near_n * slots,))],
    )(places.reshape(-1), near_index[None], table)


def layer(table, hidden, gain, ids):
    share, span_cols = table.shape
    tok = hidden.shape[0]
    far_n, near_n = lax.axis_size(FAR), lax.axis_size(NEAR)
    voc_cols = span_cols // (far_n * near_n)
    width = share * far_n * near_n
    group_index = lax.axis_index(GROUP)
    vocab_index = lax.axis_index(VOCAB)
    depth = lax.axis_index(FAR)
    steps = far_n // 2

    core = lax.axis_index("core")
    cores = lax.axis_size("core")
    offsets = [[steps - j for j in range(steps)], [j - steps + 1 for j in range(steps)]]
    places = (depth + jnp.array(offsets, jnp.int32)) % far_n
    early = steps // 2

    fill = jnp.broadcast_to(gain[:, None], (share, LANES - tok))
    both = jnp.concatenate([hidden.T, fill], axis=1)
    near_index = lax.axis_index(NEAR)
    first = arrange(table, places[:, :early], near_index, near_n, False)
    both = lax.all_gather(both, NEAR, axis=0, tiled=True)
    first, both = lax.optimization_barrier((first, both))
    swapped = jnp.zeros((near_n * share, first[0].shape[1]), table.dtype)
    for k in range(near_n):
        slab = first[k]
        if k:
            slab = lax.ppermute(slab, NEAR, [(i, i ^ k) for i in range(near_n)])
        swapped = lax.dynamic_update_slice(swapped, slab, ((near_index ^ k) * share, 0))
    first = swapped

    both = both.astype(jnp.float32)
    states, gains = both[:, :tok], both[:, tok : tok + 1]
    squares = jnp.sum(states * states, axis=0)
    squares, late_table = lax.optimization_barrier((squares, table))
    squares = copies_of(as_rows(squares), FAR).reshape(far_n, -1, 128)
    mean_sq = squares.sum(axis=0).reshape(LANES)[:tok] / width
    normed = (states * gains * lax.rsqrt(mean_sq + 1e-06)[None, :]).astype(jnp.bfloat16).T

    (second,) = arrange(late_table, places[:, early:], near_index * 0, near_n, True)
    second = lax.all_to_all(second, NEAR, split_axis=0, concat_axis=0, tiled=True)
    second = second.reshape(near_n * share, -1)

    def onward(j):
        up = [(2 * i, 2 * ((i + 1) % far_n)) for i in range(far_n)]
        down = [(2 * i + 1, 2 * ((i - 1) % far_n) + 1) for i in range(far_n)]
        return up + down if j < steps - 1 else up

    pair_cols = cores * voc_cols
    streams = 2
    rows = tok // streams
    came, out = [None] * streams, [None] * streams
    for j in range(steps):
        w, at = (first, j) if j < early else (second, j - early)
        w = w[:, at * pair_cols : (at + 1) * pair_cols]
        for h in range(streams):
            y = jnp.dot(normed[h * rows : (h + 1) * rows], w, preferred_element_type=jnp.float32)
            if j:
                y = y + came[h].astype(jnp.float32)
            out[h] = y.astype(jnp.bfloat16)
            came[h] = lax.ppermute(out[h], (FAR, "core"), onward(j))
    arms = jnp.concatenate([jnp.where(core == 0, c, o) for c, o in zip(came, out)])
    kept = lax.dynamic_slice_in_dim(arms, core * voc_cols, voc_cols, axis=1)
    given = lax.dynamic_slice_in_dim(arms, (1 - core) * voc_cols, voc_cols, axis=1)
    given = lax.ppermute(given, "core", [(0, 1), (1, 0)])
    logits = kept.astype(jnp.float32) + given.astype(jnp.float32)

    local_ids = ids - group_index * span_cols
    inside = jnp.logical_and(local_ids >= 0, local_ids < span_cols)
    found = jnp.take(late_table, jnp.clip(local_ids, 0, span_cols - 1), axis=1)
    found = jnp.where(inside[None, :], found, 0)
    found = copies_of(found, GROUP).reshape(-1, share, tok)
    embed = jnp.sum(found.astype(jnp.float32), axis=0)
    next_embed = (embed * math.sqrt(width)).astype(jnp.bfloat16).T

    capped = 30.0 * jnp.tanh(logits / 30.0)
    offsets = ids - (group_index * far_n * near_n + vocab_index) * voc_cols
    columns = lax.broadcasted_iota(jnp.int32, capped.shape, 1)
    pick = jnp.sum(jnp.where(columns == offsets[:, None], capped, 0.0), axis=1)
    sums = jnp.sum(jnp.exp(capped), axis=1)
    pair = jnp.concatenate([as_rows(sums), as_rows(pick)])
    for axes in (PLANE, FAR):
        pair = copies_of(pair, axes).reshape(-1, *pair.shape).sum(axis=0)
    totals, picks = pair.reshape(2, LANES)[:, :tok]
    log_total = jnp.log(totals)
    return (next_embed, capped - log_total[:, None], picks - log_total)


def solution(mesh):
    torus = Mesh(
        mesh.devices.reshape(4, 2, 16, 2, 2),
        GROUP + VOCAB,
    )
    return jax.shard_map(
        layer,
        mesh=torus,
        in_specs=(P(VOCAB, GROUP), P(None, VOCAB), P(VOCAB), P()),
        out_specs=(P(None, VOCAB), P(None, GROUP + VOCAB), P()),
        check_vma=False,
    )
```

```python
import math

import jax
import jax.numpy as jnp
from jax import lax
from jax.experimental import pallas as pl
from jax.experimental.pallas import tpu as pltpu
from jax.sharding import Mesh
from jax.sharding import PartitionSpec as P

GROUP = ("group_0", "group_1")
FAR = "depth"
NEAR = ("row", "core")
VOCAB = (FAR,) + NEAR
PLANE = GROUP + NEAR
LANES = 512


def copies_of(x, axes):
    many = jnp.broadcast_to(x[None], (lax.axis_size(axes),) + x.shape)
    return lax.all_to_all(many, axes, split_axis=0, concat_axis=0, tiled=True)


def as_rows(x):
    return jnp.pad(x, (0, LANES - x.shape[0])).reshape(LANES // 128, 128)


def arrange(table, places, near_index, near_n, joined):
    share, span_cols = table.shape
    cores, slots = places.shape
    per = span_cols // (lax.axis_size(FAR) * near_n)
    cols = per * cores

    def kernel(places_ref, near_ref, table_ref, *refs):
        sems = refs[-1]
        copies = []
        for k in range(near_n):
            out_ref = refs[0].at[k] if joined else refs[k]
            near = near_ref[0] ^ k
            core = near % cores
            for j in range(slots):
                block = places_ref[core * slots + j] * near_n + near - core
                copies.append(
                    pltpu.make_async_copy(
                        table_ref.at[:, pl.ds(pl.multiple_of(block * per, per), cols)],
                        out_ref.at[:, pl.ds(j * cols, cols)],
                        sems.at[k * slots + j],
                    )
                )
        for c in copies:
            c.start()
        for c in copies:
            c.wait()

    smem, vmem = pl.BlockSpec(memory_space=pltpu.SMEM), pl.BlockSpec(memory_space=pltpu.VMEM)
    return pl.pallas_call(
        kernel,
        in_specs=[smem, smem, pl.BlockSpec(memory_space=pltpu.HBM)],
        out_specs=[vmem] * (1 if joined else near_n),
        out_shape=[jax.ShapeDtypeStruct((near_n, share, slots * cols), table.dtype)]
        if joined
        else [jax.ShapeDtypeStruct((share, slots * cols), table.dtype)] * near_n,
        scratch_shapes=[pltpu.SemaphoreType.DMA((near_n * slots,))],
    )(places.reshape(-1), near_index[None], table)


def layer(table, hidden, gain, ids):
    share, span_cols = table.shape
    tok = hidden.shape[0]
    far_n, near_n = lax.axis_size(FAR), lax.axis_size(NEAR)
    voc_cols = span_cols // (far_n * near_n)
    width = share * far_n * near_n
    group_index = lax.axis_index(GROUP)
    vocab_index = lax.axis_index(VOCAB)
    depth = lax.axis_index(FAR)
    steps = far_n // 2

    core = lax.axis_index("core")
    cores = lax.axis_size("core")
    offsets = [[steps - j for j in range(steps)], [j - steps + 1 for j in range(steps)]]
    places = (depth + jnp.array(offsets, jnp.int32)) % far_n
    early = steps // 2

    fill = jnp.broadcast_to(gain[:, None], (share, LANES - tok))
    both = jnp.concatenate([hidden.T, fill], axis=1)
    near_index = lax.axis_index(NEAR)
    first = arrange(table, places[:, :early], near_index, near_n, False)
    both = lax.all_gather(both, NEAR, axis=0, tiled=True)
    first, both = lax.optimization_barrier((first, both))
    swapped = jnp.zeros((near_n * share, first[0].shape[1]), table.dtype)
    for k in range(near_n):
        slab = first[k]
        if k:
            slab = lax.ppermute(slab, NEAR, [(i, i ^ k) for i in range(near_n)])
        swapped = lax.dynamic_update_slice(swapped, slab, ((near_index ^ k) * share, 0))
    first = swapped

    both = both.astype(jnp.float32)
    states, gains = both[:, :tok], both[:, tok : tok + 1]
    squares = jnp.sum(states * states, axis=0)
    squares, late_table = lax.optimization_barrier((squares, table))
    squares = copies_of(as_rows(squares), FAR).reshape(far_n, -1, 128)
    mean_sq = squares.sum(axis=0).reshape(LANES)[:tok] / width
    normed = (states * gains * lax.rsqrt(mean_sq + 1e-06)[None, :]).astype(jnp.bfloat16).T

    (second,) = arrange(late_table, places[:, early:], near_index * 0, near_n, True)
    second = lax.all_to_all(second, NEAR, split_axis=0, concat_axis=0, tiled=True)
    second = second.reshape(near_n * share, -1)

    def onward(j):
        up = [(2 * i, 2 * ((i + 1) % far_n)) for i in range(far_n)]
        down = [(2 * i + 1, 2 * ((i - 1) % far_n) + 1) for i in range(far_n)]
        return up + down if j < steps - 1 else up

    pair_cols = cores * voc_cols
    streams = 2
    rows = tok // streams
    came, out = [None] * streams, [None] * streams
    for j in range(steps):
        w, at = (first, j) if j < early else (second, j - early)
        w = w[:, at * pair_cols : (at + 1) * pair_cols]
        for h in range(streams):
            y = jnp.dot(normed[h * rows : (h + 1) * rows], w, preferred_element_type=jnp.float32)
            if j:
                y = y + came[h].astype(jnp.float32)
            out[h] = y.astype(jnp.bfloat16)
            came[h] = lax.ppermute(out[h], (FAR, "core"), onward(j))
    arms = jnp.concatenate([jnp.where(core == 0, c, o) for c, o in zip(came, out)])
    kept = lax.dynamic_slice_in_dim(arms, core * voc_cols, voc_cols, axis=1)
    given = lax.dynamic_slice_in_dim(arms, (1 - core) * voc_cols, voc_cols, axis=1)
    given = lax.ppermute(given, "core", [(0, 1), (1, 0)])
    logits = kept.astype(jnp.float32) + given.astype(jnp.float32)

    local_ids = ids - group_index * span_cols
    inside = jnp.logical_and(local_ids >= 0, local_ids < span_cols)
    found = jnp.take(late_table, jnp.clip(local_ids, 0, span_cols - 1), axis=1)
    found = jnp.where(inside[None, :], found, 0)
    for axis, bit in (("group_0", 1), ("group_0", 2), ("group_1", 1)):
        pairs = [(q, q ^ bit) for q in range(lax.axis_size(axis))]
        other = lax.ppermute(found, axis, pairs)
        found = found + other
    next_embed = (found.astype(jnp.float32) * math.sqrt(width)).astype(jnp.bfloat16).T

    capped = 30.0 * jnp.tanh(logits / 30.0)
    offsets = ids - (group_index * far_n * near_n + vocab_index) * voc_cols
    columns = lax.broadcasted_iota(jnp.int32, capped.shape, 1)
    pick = jnp.sum(jnp.where(columns == offsets[:, None], capped, 0.0), axis=1)
    sums = jnp.sum(jnp.exp(capped), axis=1)
    pair = jnp.concatenate([as_rows(sums), as_rows(pick)])
    for axes in (PLANE, FAR):
        pair = copies_of(pair, axes).reshape(-1, *pair.shape).sum(axis=0)
    totals, picks = pair.reshape(2, LANES)[:, :tok]
    log_total = jnp.log(totals)
    return (next_embed, capped - log_total[:, None], picks - log_total)


def solution(mesh):
    torus = Mesh(
        mesh.devices.reshape(4, 2, 16, 2, 2),
        GROUP + VOCAB,
    )
    return jax.shard_map(
        layer,
        mesh=torus,
        in_specs=(P(VOCAB, GROUP), P(None, VOCAB), P(VOCAB), P()),
        out_specs=(P(None, VOCAB), P(None, GROUP + VOCAB), P()),
        check_vma=False,
    )
```
